32 devices in a mesh: ens: 4 (over y, x), fsdp: 2 (over core), model: 4 (over z).
Axes of the slice: x: 2, y: 2, z: 4, core: 2. Of those that a mesh axis runs over, the one named last changes fastest.
Arguments:
- weight_gate: bfloat16 [8192, 8192], P(('ens', 'fsdp'), 'model'), parts along dimension 0, may hold values from -0.125 to 0.125
- low_gate: bfloat16 [8192, 32], P(('ens', 'fsdp')), parts along dimension 0, may hold values from -0.125 to 0.125
- high_gate: bfloat16 [128, 8192], P('ens', 'model'), parts along dimension 0, may hold values from -1 to 1
- weight_up: bfloat16 [8192, 8192], P(('ens', 'fsdp'), 'model'), parts along dimension 0, may hold values from -0.125 to 0.125
- low_up: bfloat16 [8192, 32], P(('ens', 'fsdp')), parts along dimension 0, may hold values from -0.125 to 0.125
- high_up: bfloat16 [128, 8192], P('ens', 'model'), parts along dimension 0, may hold values from -1 to 1
- norm_train: float32 [8192], P(('ens', 'fsdp', 'model')), parts along dimension 0, may hold values from 0.25 to 1.75
- norm_step: float32 [8192], P(('ens', 'fsdp', 'model')), parts along dimension 0, may hold values from -0.3 to 0.3
Outputs:
- final_gate: bfloat16 [32768, 2048], P(('ens', 'model')), parts along dimension 0
- final_up: bfloat16 [32768, 2048], P(('ens', 'model')), parts along dimension 0
- serve_norm: bfloat16 [8192], P('ens'), parts along dimension 0
The draws below stay inside these ranges and needn't reach their ends.
There are 4 independent parts, one for each index of `ens`. The reference program is written for one: setup_inputs(seed, part) draws one part's arguments, and reference() takes and returns one part's arrays. A program takes and returns all parts, laid end to end along the dimension named above; each array names one. Nothing has to cross between parts.
All inputs are finite; a program needn't handle non-finite values.
Results may differ from the reference program's by a relative error of at most 0.001.
Values may be sent and summed in bfloat16 or wider, within the bound.
A program may use at most 128 MiB of HBM per device.

```python
import jax
import jax.numpy as jnp

D_MODEL = 2048
D_INNER = 8192
RANK = 32


def steps_of(own_key, shape, cuts, least, high):
    def one(dim, blocks):
        steps = jax.random.uniform(jax.random.fold_in(jax.random.fold_in(own_key, 6), dim), (blocks,), jnp.float32, least / len(cuts), high / len(cuts))
        return jnp.repeat(jnp.exp(steps), shape[dim] // blocks).reshape((-1,) + (1,) * (len(shape) - dim - 1))

    gain = one(*cuts[0])
    for cut in cuts[1:]:
        gain = gain * one(*cut)
    return gain


def bell_draw(own_key, shape, spread, limit, shards=(), held_as=jnp.bfloat16):
    loudness = steps_of(own_key, shape, shards, -0.22, 0.18) if shards else 1.0
    values = jax.random.normal(own_key, shape, jnp.float32) * spread * loudness
    return jnp.minimum(jnp.maximum(values, -limit), limit).astype(held_as)


def setup_inputs(seed: int = 0, part: int = 0) -> dict:
    keys = jax.random.split(jax.random.key(seed), 9)
    part_keys = jax.random.split(jax.random.fold_in(keys[8], part), 9)
    weight_gate = bell_draw(part_keys[0], (D_MODEL, D_INNER), D_MODEL ** -0.5, 0.125, ((0, 2), (1, 4)))
    low_gate = bell_draw(part_keys[1], (D_MODEL, RANK), D_MODEL ** -0.5, 0.125, ((0, 2),))
    high_gate = bell_draw(part_keys[2], (RANK, D_INNER), RANK ** -0.5, 1.0, ((1, 4),))
    weight_up = bell_draw(part_keys[3], (D_MODEL, D_INNER), D_MODEL ** -0.5, 0.125, ((0, 2), (1, 4)))
    low_up = bell_draw(part_keys[4], (D_MODEL, RANK), D_MODEL ** -0.5, 0.125, ((0, 2),))
    high_up = bell_draw(part_keys[5], (RANK, D_INNER), RANK ** -0.5, 1.0, ((1, 4),))
    norm_train = jnp.clip(1.0 + 0.15 * jax.random.normal(part_keys[6], (D_MODEL,), jnp.float32), 0.25, 1.75)
    norm_step = jnp.clip(jax.random.uniform(part_keys[7], (D_MODEL,), jnp.float32, -0.3, 0.3) * steps_of(part_keys[7], (D_MODEL,), ((0, 8),), -0.4, 0.0), -0.3, 0.3)
    return {"weight_gate": weight_gate, "low_gate": low_gate, "high_gate": high_gate, "weight_up": weight_up, "low_up": low_up, "high_up": high_up, "norm_train": norm_train, "norm_step": norm_step}


mix_rate = 2.0


def reference(weight_gate, low_gate, high_gate, weight_up, low_up, high_up, norm_train, norm_step):
    result_gate = weight_gate.astype(jnp.float32) + mix_rate * jnp.dot(low_gate, high_gate, preferred_element_type=jnp.float32)
    result_up = weight_up.astype(jnp.float32) + mix_rate * jnp.dot(low_up, high_up, preferred_element_type=jnp.float32)
    final_gate = result_gate.T.astype(jnp.bfloat16)
    final_up = result_up.T.astype(jnp.bfloat16)
    serve_norm = (norm_train + norm_step).astype(jnp.bfloat16)
    return final_gate, final_up, serve_norm
```

```python
import functools

import jax
import jax.numpy as jnp
from jax import lax
from jax.experimental import pallas as pl
from jax.experimental.pallas import tpu as pltpu
from jax.sharding import PartitionSpec as P

mix_rate = 2.0


def merge(weight, low, high):
    product = lax.dot_general(
        high, low, (((0,), (0,)), ((), ())), preferred_element_type=jnp.float32
    )
    return (weight.T.astype(jnp.float32) + mix_rate * product).astype(jnp.bfloat16)


def merge_kernel(count, where_ref, *refs):
    outs = refs[len(refs) - count:]
    for i, out in enumerate(outs):
        weight, low, high = refs[3 * i: 3 * i + 3]
        out[...] = merge(weight[...], low[...], high[...])


def merged(where, groups, fsdp, held=None):
    rows, columns = groups[0][0].shape
    rank = groups[0][1].shape[0]
    tile = min(columns, 256)
    count = len(groups)
    in_specs, operands = [], []
    for group in groups:
        in_specs += [
            pl.BlockSpec((rows, tile), lambda j, w: (0, j)),
            pl.BlockSpec((rank, rows), lambda j, w: (0, 0)),
            pl.BlockSpec((rank, tile), lambda j, w: (0, j)),
        ]
        operands += list(group)
    aliases = {}
    if held is not None:
        for i, array in enumerate(held):
            aliases[1 + len(operands)] = i
            operands.append(array)
            in_specs.append(pl.BlockSpec(memory_space=pl.ANY))
    return pl.pallas_call(
        functools.partial(merge_kernel, count),
        out_shape=[jax.ShapeDtypeStruct((columns, rows * fsdp), jnp.bfloat16)] * count,
        grid_spec=pltpu.PrefetchScalarGridSpec(
            num_scalar_prefetch=1,
            grid=(columns // tile,),
            in_specs=in_specs,
            out_specs=[pl.BlockSpec((tile, rows), lambda j, w: (j, w[0]))] * count,
        ),
        input_output_aliases=aliases,
        cost_estimate=pl.CostEstimate(
            flops=2 * count * rows * columns * rank,
            bytes_accessed=4 * count * rows * columns,
            transcendentals=0,
        ),
    )(where, *operands)


def body(fsdp, weight_gate, low_gate, high_gate, weight_up, low_up, high_up, norm_train, norm_step):
    me = lax.axis_index("fsdp")
    low_gate, low_up = low_gate.T, low_up.T
    moved = []
    for step in range(1, fsdp):
        pairs = [(i, (i + step) % fsdp) for i in range(fsdp)]
        moved.append([lax.ppermute(a, "fsdp", pairs) for a in (low_gate, low_up, weight_gate, weight_up)])
    gate, up = merged(
        me[None], [(weight_gate, low_gate, high_gate), (weight_up, low_up, high_up)], fsdp
    )
    serve_norm = lax.all_gather(
        (norm_train + norm_step).astype(jnp.bfloat16), ("fsdp", "model"), axis=0, tiled=True
    )
    for step, (its_low_gate, its_low_up, its_gate, its_up) in enumerate(moved, 1):
        where = lax.rem(me + (fsdp - step), fsdp)[None]
        (gate,) = merged(where, [(its_gate, its_low_gate, high_gate)], fsdp, [gate])
        (up,) = merged(where, [(its_up, its_low_up, high_up)], fsdp, [up])
    return gate, up, serve_norm


def solution(mesh):
    return jax.shard_map(
        functools.partial(body, mesh.shape["fsdp"]),
        mesh=mesh,
        in_specs=(
            P(("ens", "fsdp"), "model"),
            P(("ens", "fsdp"), None),
            P("ens", "model"),
            P(("ens", "fsdp"), "model"),
            P(("ens", "fsdp"), None),
            P("ens", "model"),
            P(("ens", "fsdp", "model")),
            P(("ens", "fsdp", "model")),
        ),
        out_specs=(P(("ens", "model"), None), P(("ens", "model"), None), P("ens")),
        check_vma=False,
    )
```

```python
import functools

import jax
import jax.numpy as jnp
from jax import lax
from jax.experimental import pallas as pl
from jax.experimental.pallas import tpu as pltpu
from jax.sharding import PartitionSpec as P

mix_rate = 2.0
MIB = 2 ** 20


def merge(weight, low, high):
    product = lax.dot_general(
        high, low, (((0,), (0,)), ((), ())), preferred_element_type=jnp.float32
    )
    return (weight.T.astype(jnp.float32) + mix_rate * product).astype(jnp.bfloat16)


def exchange_kernel(
    sizes, tile,
    gate, low_gate, high_gate, up, low_up, high_up, norm_train, norm_step,
    own_gate, own_up, their_gate, their_low, norm_all,
    gate_held, up_held, low_held, high_held, gate_landed,
    read_sem, small_sem, norm_own_sem, norm_send, norm_recv, low_send, low_recv, gate_send, gate_recv,
):
    fsdp, model = sizes
    count = fsdp * model
    rows, columns = gate.shape
    steps = columns // tile
    row, column = lax.axis_index("fsdp"), lax.axis_index("model")
    barrier = pltpu.get_barrier_semaphore()

    def peer(shift):
        return {
            "fsdp": lax.rem(row + shift // model, fsdp),
            "model": lax.rem(column + shift % model, model),
        }

    for shift in range(1, count):
        pl.semaphore_signal(
            barrier, inc=1, device_id=peer(shift), device_id_type=pl.DeviceIdType.MESH
        )

    lows, norms = (low_gate, low_up), (norm_train, norm_step)
    local = [
        pltpu.make_async_copy(source, target, small_sem.at[i])
        for i, (source, target) in enumerate((
            (low_gate, low_held.at[0]), (high_gate, high_held.at[0]),
            (low_up, low_held.at[1]), (high_up, high_held.at[1]),
        ))
    ]
    place = row * model + column
    keep = [
        pltpu.make_async_copy(norms[i], norm_all.at[i, place], norm_own_sem.at[i]) for i in range(2)
    ]
    reads = [
        [
            pltpu.make_async_copy(
                source.at[:, pl.ds(j * tile, tile)], target.at[j], read_sem.at[i, j]
            )
            for j in range(steps)
        ]
        for i, (source, target) in enumerate(((up, up_held), (gate, gate_held)))
    ]
    for copy in local + keep + reads[0] + reads[1]:
        copy.start()

    pl.semaphore_wait(barrier, count - 1)
    sent = []

    def send(source, target, send_sem, recv_sem, device):
        copy = pltpu.make_async_remote_copy(
            src_ref=source, dst_ref=target, send_sem=send_sem, recv_sem=recv_sem,
            device_id=device, device_id_type=pl.DeviceIdType.MESH,
        )
        copy.start()
        sent.append(copy)
        return copy

    norm_copies, low_copies, gate_copies = [], [], []
    for shift in range(1, count):
        for i in range(2):
            norm_copies.append(send(
                norms[i], norm_all.at[i, place],
                norm_send.at[i, shift], norm_recv.at[i, shift], peer(shift),
            ))
    for step in range(1, fsdp):
        for i in range(2):
            low_copies.append(send(
                lows[i], their_low.at[i, step - 1],
                low_send.at[i, step], low_recv.at[i, step], peer(step * model),
            ))
    for step in range(1, fsdp):
        for j in range(steps):
            gate_copies.append(send(
                gate.at[:, pl.ds(j * tile, tile)], gate_landed.at[step - 1, j],
                gate_send.at[step, j], gate_recv.at[step, j], peer(step * model),
            ))

    for copy in local:
        copy.wait()
    for i, (held, made) in enumerate(((up_held, own_up), (gate_held, own_gate))):
        for j in range(steps):
            piece = pl.ds(j * tile, tile)
            reads[i][j].wait()
            made[piece, :] = merge(held[j], low_held[1 - i], high_held[1 - i, :, piece])
    for copy in low_copies:
        copy.wait_recv()
    for step in range(1, fsdp):
        for j in range(steps):
            piece = pl.ds(j * tile, tile)
            gate_copies[(step - 1) * steps + j].wait_recv()
            their_gate[step - 1, piece, :] = merge(
                gate_landed[step - 1, j], their_low[0, step - 1], high_held[0, :, piece]
            )
    for copy in norm_copies:
        copy.wait_recv()
    for copy in keep:
        copy.wait()
    for copy in sent:
        copy.wait_send()


def exchange(sizes, gate, low_gate, high_gate, up, low_up, high_up, norm_train, norm_step):
    fsdp, model = sizes
    count = fsdp * model
    rows, columns = gate.shape
    rank = low_gate.shape[0]
    tile = min(columns, 256)
    steps = columns // tile
    vmem = pl.BlockSpec(memory_space=pltpu.VMEM)
    dma = pltpu.SemaphoreType.DMA
    half, kind = jnp.bfloat16, pltpu.VMEM
    return pl.pallas_call(
        functools.partial(exchange_kernel, sizes, tile),
        out_shape=[
            kind((columns, rows), half),
            kind((columns, rows), half),
            kind((fsdp - 1, columns, rows), half),
            kind((2, fsdp - 1, rank, rows), half),
            kind((2, count) + norm_train.shape, jnp.float32),
        ],
        in_specs=[pl.BlockSpec(memory_space=pltpu.HBM)] * 8,
        out_specs=[vmem] * 5,
        scratch_shapes=[
            pltpu.VMEM((steps, rows, tile), half),
            pltpu.VMEM((steps, rows, tile), half),
            pltpu.VMEM((2, rank, rows), half),
            pltpu.VMEM((2, rank, columns), half),
            pltpu.VMEM((fsdp - 1, steps, rows, tile), half),
            dma((2, steps)), dma((4,)), dma((2,)),
            dma((2, count)), dma((2, count)),
            dma((2, fsdp)), dma((2, fsdp)),
            dma((fsdp, steps)), dma((fsdp, steps)),
        ],
        compiler_params=pltpu.CompilerParams(
            collective_id=0, has_side_effects=True, vmem_limit_bytes=20 * MIB
        ),
        cost_estimate=pl.CostEstimate(
            flops=4 * fsdp * rows * columns * rank,
            bytes_accessed=20 * rows * columns,
            transcendentals=0,
        ),
    )(*[in_hbm(a) for a in (gate, low_gate, high_gate, up, low_up, high_up, norm_train, norm_step)])


def place_kernel(fsdp, tile, own_gate, own_up, their_gate, norm_all, gate, up, serve_norm, sem):
    columns, rows = own_gate.shape
    me = lax.axis_index("fsdp")
    steps = columns // tile
    others = their_gate.shape[0]
    copies = []
    parts = [(own_gate, gate, 0), (own_up, up, 0)]
    parts += [(their_gate.at[i], gate, i + 1) for i in range(others)]
    for i, (source, target, k) in enumerate(parts):
        column = pl.multiple_of(lax.rem(me + (fsdp - k), fsdp) * rows, rows)
        for j in range(steps):
            piece = pl.ds(j * tile, tile)
            copy = pltpu.make_async_copy(
                source.at[piece], target.at[piece, pl.ds(column, rows)], sem.at[i, j]
            )
            copy.start()
            copies.append(copy)
    size = norm_all.shape[3]
    for i in range(norm_all.shape[1]):
        total = norm_all[0, i, 0, :] + norm_all[1, i, 0, :]
        serve_norm[pl.ds(i * size, size)] = total.astype(serve_norm.dtype)
    for copy in copies:
        copy.wait()


def in_vmem(array):
    return pltpu.with_memory_space_constraint(array, pltpu.VMEM)


def in_hbm(array):
    return pltpu.with_memory_space_constraint(array, pltpu.HBM)


def placed(own_gate, own_up, their_gate, norm_all):
    columns, rows = own_gate.shape
    others = their_gate.shape[0]
    tile = min(columns, 256)
    vmem, anywhere = pl.BlockSpec(memory_space=pltpu.VMEM), pl.BlockSpec(memory_space=pl.ANY)
    return pl.pallas_call(
        functools.partial(place_kernel, others + 1, tile),
        out_shape=[jax.ShapeDtypeStruct((columns, rows * (others + 1)), own_gate.dtype)] * 2
        + [jax.ShapeDtypeStruct((norm_all[0].size,), jnp.bfloat16)],
        in_specs=[vmem] * 4,
        out_specs=[anywhere] * 2 + [vmem],
        scratch_shapes=[pltpu.SemaphoreType.DMA((2 + others, columns // tile))],
        compiler_params=pltpu.CompilerParams(vmem_limit_bytes=2 * MIB),
        cost_estimate=pl.CostEstimate(
            flops=0, bytes_accessed=2 * (2 + others) * rows * columns, transcendentals=0
        ),
    )(in_vmem(own_gate), in_vmem(own_up), in_vmem(their_gate), in_vmem(norm_all))


def their_kernel(fsdp, step, tile, weight, low_ref, high, held_ref, out, made, write_sem):
    low = low_ref.at[1, step - 1]
    rows, columns = weight.shape
    steps = columns // tile
    from_device = lax.rem(lax.axis_index("fsdp") + (fsdp - step), fsdp)
    column = pl.multiple_of(from_device * rows, rows)

    def write(j):
        return pltpu.make_async_copy(
            made.at[j], out.at[pl.ds(j * tile, tile), pl.ds(column, rows)], write_sem.at[j]
        )

    for j in range(steps):
        piece = pl.ds(j * tile, tile)
        made[j] = merge(weight[:, piece], low[...], high[:, piece])
        write(j).start()
    for j in range(steps):
        write(j).wait()


def their_part(step, weight, low, high, held):
    rows, columns = weight.shape
    rank = low.shape[2]
    tile = min(columns, 256)
    steps = columns // tile
    vmem, anywhere = pl.BlockSpec(memory_space=pltpu.VMEM), pl.BlockSpec(memory_space=pl.ANY)
    return pl.pallas_call(
        functools.partial(their_kernel, held.shape[1] // rows, step, tile),
        out_shape=jax.ShapeDtypeStruct(held.shape, held.dtype),
        in_specs=[vmem, vmem, vmem, anywhere],
        out_specs=anywhere,
        scratch_shapes=[
            pltpu.VMEM((steps, tile, rows), jnp.bfloat16),
            pltpu.SemaphoreType.DMA((steps,)),
        ],
        input_output_aliases={3: 0},
        compiler_params=pltpu.CompilerParams(vmem_limit_bytes=12 * MIB),
        cost_estimate=pl.CostEstimate(
            flops=2 * rows * columns * rank, bytes_accessed=2 * rows * columns, transcendentals=0
        ),
    )(in_vmem(weight), in_vmem(low), high, held)


def body(sizes, weight_gate, low_gate, high_gate, weight_up, low_up, high_up, norm_train, norm_step):
    fsdp, model = sizes
    own_gate, own_up, their_gate, their_low, norm = exchange(
        sizes, weight_gate, low_gate.T, high_gate, weight_up, low_up.T, high_up,
        norm_train.reshape(1, -1), norm_step.reshape(1, -1),
    )
    weight_up, own_gate = lax.optimization_barrier((weight_up, own_gate))
    moved = [
        lax.ppermute(weight_up, "fsdp", [(i, (i + step) % fsdp) for i in range(fsdp)])
        for step in range(1, fsdp)
    ]
    gate, up, serve_norm = placed(own_gate, own_up, their_gate, norm)
    for step, their_up in enumerate(moved, 1):
        up = their_part(step, their_up, their_low, high_up, up)
    return gate, up, serve_norm


def solution(mesh):
    return jax.shard_map(
        functools.partial(body, (mesh.shape["fsdp"], mesh.shape["model"])),
        mesh=mesh,
        in_specs=(
            P(("ens", "fsdp"), "model"),
            P(("ens", "fsdp"), None),
            P("ens", "model"),
            P(("ens", "fsdp"), "model"),
            P(("ens", "fsdp"), None),
            P("ens", "model"),
            P(("ens", "fsdp", "model")),
            P(("ens", "fsdp", "model")),
        ),
        out_specs=(P(("ens", "model"), None), P(("ens", "model"), None), P("ens")),
        check_vma=False,
    )
```

```python
import functools

import jax
import jax.numpy as jnp
from jax import lax
from jax.experimental import pallas as pl
from jax.experimental.pallas import tpu as pltpu
from jax.sharding import PartitionSpec as P

mix_rate = 2.0
MIB = 2 ** 20


def merge(weight, low, high):
    product = lax.dot_general(
        high, low, (((0,), (0,)), ((), ())), preferred_element_type=jnp.float32
    )
    return (weight.T.astype(jnp.float32) + mix_rate * product).astype(jnp.bfloat16)


def exchange_kernel(
    sizes, tile,
    gate, low_gate, high_gate, up, low_up, high_up, norm_train, norm_step,
    own_gate, own_up, their_gate, their_low, norm_all,
    gate_held, up_held, low_held, high_held, gate_landed,
    read_sem, small_sem, norm_own_sem, norm_send, norm_recv, low_send, low_recv, gate_send, gate_recv,
):
    fsdp, model = sizes
    count = fsdp * model
    rows, columns = gate.shape
    steps = rows // tile
    row, column = lax.axis_index("fsdp"), lax.axis_index("model")
    barrier = pltpu.get_barrier_semaphore()

    def peer(shift):
        return {
            "fsdp": lax.rem(row + shift // model, fsdp),
            "model": lax.rem(column + shift % model, model),
        }

    for shift in range(1, count):
        pl.semaphore_signal(
            barrier, inc=1, device_id=peer(shift), device_id_type=pl.DeviceIdType.MESH
        )

    lows, norms = (low_gate, low_up), (norm_train, norm_step)
    local = [
        pltpu.make_async_copy(source, target, small_sem.at[i])
        for i, (source, target) in enumerate((
            (low_gate, low_held.at[0]), (high_gate, high_held.at[0]),
            (low_up, low_held.at[1]), (high_up, high_held.at[1]),
        ))
    ]
    place = row * model + column
    keep = [
        pltpu.make_async_copy(norms[i], norm_all.at[i, place], norm_own_sem.at[i]) for i in range(2)
    ]
    reads = [
        [
            pltpu.make_async_copy(
                source.at[pl.ds(j * tile, tile)], target.at[j], read_sem.at[i, j]
            )
            for j in range(steps)
        ]
        for i, (source, target) in enumerate(((gate, gate_held), (up, up_held)))
    ]
    for copy in local + keep + reads[0] + reads[1]:
        copy.start()

    pl.semaphore_wait(barrier, count - 1)
    sent = []

    def send(source, target, send_sem, recv_sem, device):
        copy = pltpu.make_async_remote_copy(
            src_ref=source, dst_ref=target, send_sem=send_sem, recv_sem=recv_sem,
            device_id=device, device_id_type=pl.DeviceIdType.MESH,
        )
        copy.start()
        sent.append(copy)
        return copy

    norm_copies, low_copies, gate_copies = [], [], []
    for shift in range(1, count):
        for i in range(2):
            norm_copies.append(send(
                norms[i], norm_all.at[i, place],
                norm_send.at[i, shift], norm_recv.at[i, shift], peer(shift),
            ))
    for step in range(1, fsdp):
        for i in range(2):
            low_copies.append(send(
                lows[i], their_low.at[i, step - 1],
                low_send.at[i, step], low_recv.at[i, step], peer(step * model),
            ))
    for step in range(1, fsdp):
        for j in range(steps):
            if step == 1:
                reads[0][j].wait()
            gate_copies.append(send(
                gate_held.at[j], gate_landed.at[step - 1, j],
                gate_send.at[step, j], gate_recv.at[step, j], peer(step * model),
            ))

    for copy in local:
        copy.wait()
    for i, (held, made) in enumerate(((gate_held, own_gate), (up_held, own_up))):
        for j in range(steps):
            piece = pl.ds(j * tile, tile)
            if i == 1:
                reads[i][j].wait()
            made[:, piece] = merge(held[j], low_held[i, :, piece], high_held[i])
    for copy in low_copies:
        copy.wait_recv()
    for step in range(1, fsdp):
        for j in range(steps):
            piece = pl.ds(j * tile, tile)
            gate_copies[(step - 1) * steps + j].wait_recv()
            their_gate[step - 1, :, piece] = merge(
                gate_landed[step - 1, j], their_low[0, step - 1, :, piece], high_held[0]
            )
    for copy in norm_copies:
        copy.wait_recv()
    for copy in keep:
        copy.wait()
    for copy in sent:
        copy.wait_send()


def exchange(sizes, gate, low_gate, high_gate, up, low_up, high_up, norm_train, norm_step):
    fsdp, model = sizes
    count = fsdp * model
    rows, columns = gate.shape
    rank = low_gate.shape[0]
    tile = min(rows, 256)
    steps = rows // tile
    vmem = pl.BlockSpec(memory_space=pltpu.VMEM)
    dma = pltpu.SemaphoreType.DMA
    half, kind = jnp.bfloat16, pltpu.VMEM
    return pl.pallas_call(
        functools.partial(exchange_kernel, sizes, tile),
        out_shape=[
            kind((columns, rows), half),
            kind((columns, rows), half),
            kind((fsdp - 1, columns, rows), half),
            kind((2, fsdp - 1, rank, rows), half),
            kind((2, count) + norm_train.shape, jnp.float32),
        ],
        in_specs=[pl.BlockSpec(memory_space=pltpu.HBM)] * 8,
        out_specs=[vmem] * 5,
        scratch_shapes=[
            pltpu.VMEM((steps, tile, columns), half),
            pltpu.VMEM((steps, tile, columns), half),
            pltpu.VMEM((2, rank, rows), half),
            pltpu.VMEM((2, rank, columns), half),
            pltpu.VMEM((fsdp - 1, steps, tile, columns), half),
            dma((2, steps)), dma((4,)), dma((2,)),
            dma((2, count)), dma((2, count)),
            dma((2, fsdp)), dma((2, fsdp)),
            dma((fsdp, steps)), dma((fsdp, steps)),
        ],
        compiler_params=pltpu.CompilerParams(
            collective_id=0, has_side_effects=True, vmem_limit_bytes=20 * MIB
        ),
        cost_estimate=pl.CostEstimate(
            flops=4 * fsdp * rows * columns * rank,
            bytes_accessed=20 * rows * columns,
            transcendentals=0,
        ),
    )(*[in_hbm(a) for a in (gate, low_gate, high_gate, up, low_up, high_up, norm_train, norm_step)])


def place_kernel(fsdp, tile, own_gate, own_up, their_gate, norm_all, gate, up, serve_norm, sem):
    columns, rows = own_gate.shape
    me = lax.axis_index("fsdp")
    steps = columns // tile
    others = their_gate.shape[0]
    copies = []
    parts = [(own_gate, gate, 0), (own_up, up, 0)]
    parts += [(their_gate.at[i], gate, i + 1) for i in range(others)]
    for i, (source, target, k) in enumerate(parts):
        column = pl.multiple_of(lax.rem(me + (fsdp - k), fsdp) * rows, rows)
        for j in range(steps):
            piece = pl.ds(j * tile, tile)
            copy = pltpu.make_async_copy(
                source.at[piece], target.at[piece, pl.ds(column, rows)], sem.at[i, j]
            )
            copy.start()
            copies.append(copy)
    size = norm_all.shape[3]
    for i in range(norm_all.shape[1]):
        total = norm_all[0, i, 0, :] + norm_all[1, i, 0, :]
        serve_norm[pl.ds(i * size, size)] = total.astype(serve_norm.dtype)
    for copy in copies:
        copy.wait()


def in_vmem(array):
    return pltpu.with_memory_space_constraint(array, pltpu.VMEM)


def in_hbm(array):
    return pltpu.with_memory_space_constraint(array, pltpu.HBM)


def placed(own_gate, own_up, their_gate, norm_all):
    columns, rows = own_gate.shape
    others = their_gate.shape[0]
    tile = min(columns, 256)
    vmem, anywhere = pl.BlockSpec(memory_space=pltpu.VMEM), pl.BlockSpec(memory_space=pl.ANY)
    return pl.pallas_call(
        functools.partial(place_kernel, others + 1, tile),
        out_shape=[jax.ShapeDtypeStruct((columns, rows * (others + 1)), own_gate.dtype)] * 2
        + [jax.ShapeDtypeStruct((norm_all[0].size,), jnp.bfloat16)],
        in_specs=[vmem] * 4,
        out_specs=[anywhere] * 2 + [vmem],
        scratch_shapes=[pltpu.SemaphoreType.DMA((2 + others, columns // tile))],
        compiler_params=pltpu.CompilerParams(vmem_limit_bytes=2 * MIB),
        cost_estimate=pl.CostEstimate(
            flops=0, bytes_accessed=2 * (2 + others) * rows * columns, transcendentals=0
        ),
    )(in_vmem(own_gate), in_vmem(own_up), in_vmem(their_gate), in_vmem(norm_all))


def their_kernel(fsdp, step, tile, weight, low_ref, high, held_ref, out, made, write_sem):
    low = low_ref.at[1, step - 1]
    rows, columns = weight.shape
    steps = columns // tile
    from_device = lax.rem(lax.axis_index("fsdp") + (fsdp - step), fsdp)
    column = pl.multiple_of(from_device * rows, rows)

    def write(j):
        return pltpu.make_async_copy(
            made.at[j], out.at[pl.ds(j * tile, tile), pl.ds(column, rows)], write_sem.at[j]
        )

    for j in range(steps):
        piece = pl.ds(j * tile, tile)
        made[j] = merge(weight[:, piece], low[...], high[:, piece])
        write(j).start()
    for j in range(steps):
        write(j).wait()


def their_part(step, weight, low, high, held):
    rows, columns = weight.shape
    rank = low.shape[2]
    tile = min(columns, 256)
    steps = columns // tile
    vmem, anywhere = pl.BlockSpec(memory_space=pltpu.VMEM), pl.BlockSpec(memory_space=pl.ANY)
    return pl.pallas_call(
        functools.partial(their_kernel, held.shape[1] // rows, step, tile),
        out_shape=jax.ShapeDtypeStruct(held.shape, held.dtype),
        in_specs=[vmem, vmem, vmem, anywhere],
        out_specs=anywhere,
        scratch_shapes=[
            pltpu.VMEM((steps, tile, rows), jnp.bfloat16),
            pltpu.SemaphoreType.DMA((steps,)),
        ],
        input_output_aliases={3: 0},
        compiler_params=pltpu.CompilerParams(vmem_limit_bytes=12 * MIB),
        cost_estimate=pl.CostEstimate(
            flops=2 * rows * columns * rank, bytes_accessed=2 * rows * columns, transcendentals=0
        ),
    )(in_vmem(weight), in_vmem(low), high, held)


def body(sizes, weight_gate, low_gate, high_gate, weight_up, low_up, high_up, norm_train, norm_step):
    fsdp, model = sizes
    own_gate, own_up, their_gate, their_low, norm = exchange(
        sizes, weight_gate, low_gate.T, high_gate, weight_up, low_up.T, high_up,
        norm_train.reshape(1, -1), norm_step.reshape(1, -1),
    )
    weight_up, own_gate = lax.optimization_barrier((weight_up, own_gate))
    moved = [
        lax.ppermute(weight_up, "fsdp", [(i, (i + step) % fsdp) for i in range(fsdp)])
        for step in range(1, fsdp)
    ]
    gate, up, serve_norm = placed(own_gate, own_up, their_gate, norm)
    for step, their_up in enumerate(moved, 1):
        up = their_part(step, their_up, their_low, high_up, up)
    return gate, up, serve_norm


def solution(mesh):
    return jax.shard_map(
        functools.partial(body, (mesh.shape["fsdp"], mesh.shape["model"])),
        mesh=mesh,
        in_specs=(
            P(("ens", "fsdp"), "model"),
            P(("ens", "fsdp"), None),
            P("ens", "model"),
            P(("ens", "fsdp"), "model"),
            P(("ens", "fsdp"), None),
            P("ens", "model"),
            P(("ens", "fsdp", "model")),
            P(("ens", "fsdp", "model")),
        ),
        out_specs=(P(("ens", "model"), None), P(("ens", "model"), None), P("ens")),
        check_vma=False,
    )
```

```python
import functools

import jax
import jax.numpy as jnp
from jax import lax
from jax.experimental import pallas as pl
from jax.experimental.pallas import tpu as pltpu
from jax.sharding import PartitionSpec as P

mix_rate = 2.0
MIB = 2 ** 20


def in_vmem(array):
    return pltpu.with_memory_space_constraint(array, pltpu.VMEM)


def in_hbm(array):
    return pltpu.with_memory_space_constraint(array, pltpu.HBM)


def merge(weight, low, high):
    product = lax.dot_general(
        high, low, (((0,), (0,)), ((), ())), preferred_element_type=jnp.float32
    )
    return (weight.T.astype(jnp.float32) + mix_rate * product).astype(jnp.bfloat16)


def own_kernel(fsdp, count, tile, *refs):
    ins, outs = refs[: 3 * count], refs[3 * count: 4 * count]
    held, made, low_held, high_held, read_sem, write_sem, small_sem = refs[4 * count:]
    rows, columns = ins[0].shape
    steps = columns // tile
    column = pl.multiple_of(lax.axis_index("fsdp") * rows, rows)

    def small(i):
        return (
            pltpu.make_async_copy(ins[3 * i + 1], low_held.at[i], small_sem.at[i, 0]),
            pltpu.make_async_copy(ins[3 * i + 2], high_held.at[i], small_sem.at[i, 1]),
        )

    def read(i, j):
        return pltpu.make_async_copy(
            ins[3 * i].at[:, pl.ds(j * tile, tile)], held.at[i, j], read_sem.at[i, j]
        )

    def write(i, j):
        return pltpu.make_async_copy(
            made.at[i, j], outs[i].at[pl.ds(j * tile, tile), pl.ds(column, rows)], write_sem.at[i, j]
        )

    for i in range(count):
        for copy in small(i):
            copy.start()
        for j in range(steps):
            read(i, j).start()
    for i in range(count):
        for copy in small(i):
            copy.wait()
        for j in range(steps):
            read(i, j).wait()
            made[i, j] = merge(held[i, j], low_held[i], high_held[i, :, j * tile: (j + 1) * tile])
            write(i, j).start()
    for i in range(count):
        for j in range(steps):
            write(i, j).wait()


def own_part(groups, fsdp):
    rows, columns = groups[0][0].shape
    rank = groups[0][1].shape[0]
    tile = min(columns, 256)
    count, steps = len(groups), columns // tile
    return pl.pallas_call(
        functools.partial(own_kernel, fsdp, count, tile),
        out_shape=[jax.ShapeDtypeStruct((columns, rows * fsdp), jnp.bfloat16)] * count,
        in_specs=[pl.BlockSpec(memory_space=pltpu.HBM)] * (3 * count),
        out_specs=[pl.BlockSpec(memory_space=pl.ANY)] * count,
        scratch_shapes=[
            pltpu.VMEM((count, steps, rows, tile), jnp.bfloat16),
            pltpu.VMEM((count, steps, tile, rows), jnp.bfloat16),
            pltpu.VMEM((count, rank, rows), jnp.bfloat16),
            pltpu.VMEM((count, rank, columns), jnp.bfloat16),
            pltpu.SemaphoreType.DMA((count, steps)),
            pltpu.SemaphoreType.DMA((count, steps)),
            pltpu.SemaphoreType.DMA((count, 2)),
        ],
        compiler_params=pltpu.CompilerParams(vmem_limit_bytes=24 * MIB),
        cost_estimate=pl.CostEstimate(
            flops=2 * count * rows * columns * rank,
            bytes_accessed=4 * count * rows * columns,
            transcendentals=0,
        ),
    )(*[in_hbm(a) for group in groups for a in group])


def their_kernel(
    fsdp, step, tile,
    gate, low_gate, high_gate, up, low_up, high_up, norm_all, held_gate, held_up,
    out_gate, out_up, serve_norm, made, write_sem,
):
    rows, columns = gate.shape
    steps = columns // tile
    source = lax.rem(lax.axis_index("fsdp") + (fsdp - step), fsdp)
    column = pl.multiple_of(source * rows, rows)
    groups = ((gate, low_gate, high_gate, out_gate), (up, low_up, high_up, out_up))

    def write(i, j):
        return pltpu.make_async_copy(
            made.at[i, j],
            groups[i][3].at[pl.ds(j * tile, tile), pl.ds(column, rows)],
            write_sem.at[i, j],
        )

    for i, (weight, low, high, _) in enumerate(groups):
        for j in range(steps):
            piece = pl.ds(j * tile, tile)
            made[i, j] = merge(weight[:, piece], low[...], high[:, piece])
            write(i, j).start()
    size = norm_all.shape[3]
    for i in range(norm_all.shape[1]):
        total = norm_all[0, i, 0, :] + norm_all[1, i, 0, :]
        serve_norm[pl.ds(i * size, size)] = total.astype(serve_norm.dtype)
    for i in range(2):
        for j in range(steps):
            write(i, j).wait()


def their_part(step, groups, norm_all, held):
    rows, columns = groups[0][0].shape
    rank = groups[0][1].shape[0]
    tile = min(columns, 256)
    steps = columns // tile
    vmem, anywhere = pl.BlockSpec(memory_space=pltpu.VMEM), pl.BlockSpec(memory_space=pl.ANY)
    return pl.pallas_call(
        functools.partial(their_kernel, held[0].shape[1] // rows, step, tile),
        out_shape=[jax.ShapeDtypeStruct(a.shape, a.dtype) for a in held]
        + [jax.ShapeDtypeStruct((norm_all[0].size,), jnp.bfloat16)],
        in_specs=[vmem] * 7 + [anywhere] * 2,
        out_specs=[anywhere] * 2 + [vmem],
        scratch_shapes=[
            pltpu.VMEM((2, steps, tile, rows), jnp.bfloat16),
            pltpu.SemaphoreType.DMA((2, steps)),
        ],
        input_output_aliases={7: 0, 8: 1},
        compiler_params=pltpu.CompilerParams(vmem_limit_bytes=12 * MIB),
        cost_estimate=pl.CostEstimate(
            flops=4 * rows * columns * rank, bytes_accessed=4 * rows * columns, transcendentals=0
        ),
    )(*[in_vmem(a) for group in groups for a in group], in_vmem(norm_all), *held)


def gather_kernel(
    sizes, norm_train, norm_step, norm_all, own_sem, send_sem, recv_sem
):
    fsdp, model = sizes
    count = fsdp * model
    row, column = lax.axis_index("fsdp"), lax.axis_index("model")
    barrier = pltpu.get_barrier_semaphore()
    norms = (norm_train, norm_step)

    def peer(shift):
        return {
            "fsdp": lax.rem(row + shift // model, fsdp),
            "model": lax.rem(column + shift % model, model),
        }

    for shift in range(1, count):
        pl.semaphore_signal(
            barrier, inc=1, device_id=peer(shift), device_id_type=pl.DeviceIdType.MESH
        )

    place = row * model + column
    keep = [
        pltpu.make_async_copy(norms[i], norm_all.at[i, place], own_sem.at[i]) for i in range(2)
    ]
    for copy in keep:
        copy.start()
    pl.semaphore_wait(barrier, count - 1)
    copies = []
    for shift in range(1, count):
        for i in range(2):
            copy = pltpu.make_async_remote_copy(
                src_ref=norms[i], dst_ref=norm_all.at[i, place],
                send_sem=send_sem.at[i, shift], recv_sem=recv_sem.at[i, shift],
                device_id=peer(shift), device_id_type=pl.DeviceIdType.MESH,
            )
            copy.start()
            copies.append(copy)
    for copy in keep + copies:
        copy.wait()


def gathered(sizes, norm_train, norm_step):
    count = sizes[0] * sizes[1]
    dma = pltpu.SemaphoreType.DMA
    return pl.pallas_call(
        functools.partial(gather_kernel, sizes),
        out_shape=pltpu.VMEM((2, count) + norm_train.shape, jnp.float32),
        in_specs=[pl.BlockSpec(memory_space=pltpu.HBM)] * 2,
        out_specs=pl.BlockSpec(memory_space=pltpu.VMEM),
        scratch_shapes=[dma((2,)), dma((2, count)), dma((2, count))],
        compiler_params=pltpu.CompilerParams(
            collective_id=0, has_side_effects=True, vmem_limit_bytes=MIB
        ),
        cost_estimate=pl.CostEstimate(flops=0, bytes_accessed=10 * MIB, transcendentals=0),
    )(in_hbm(norm_train), in_hbm(norm_step))


def body(sizes, weight_gate, low_gate, high_gate, weight_up, low_up, high_up, norm_train, norm_step):
    fsdp, model = sizes
    low_gate, low_up = low_gate.T, low_up.T
    moved = []
    for step in range(1, fsdp):
        pairs = [(i, (i + step) % fsdp) for i in range(fsdp)]
        moved.append([
            lax.ppermute(a, "fsdp", pairs) for a in (low_gate, low_up, weight_gate, weight_up)
        ])
    gate, up = own_part([(weight_gate, low_gate, high_gate), (weight_up, low_up, high_up)], fsdp)
    norm_train, norm_step, gate = lax.optimization_barrier((norm_train, norm_step, gate))
    norm = gathered(sizes, norm_train.reshape(1, -1), norm_step.reshape(1, -1))
    for step, (its_low_gate, its_low_up, its_gate, its_up) in enumerate(moved, 1):
        groups = [(its_gate, its_low_gate, high_gate), (its_up, its_low_up, high_up)]
        gate, up, serve_norm = their_part(step, groups, norm, [gate, up])
    return gate, up, serve_norm


def solution(mesh):
    return jax.shard_map(
        functools.partial(body, (mesh.shape["fsdp"], mesh.shape["model"])),
        mesh=mesh,
        in_specs=(
            P(("ens", "fsdp"), "model"),
            P(("ens", "fsdp"), None),
            P("ens", "model"),
            P(("ens", "fsdp"), "model"),
            P(("ens", "fsdp"), None),
            P("ens", "model"),
            P(("ens", "fsdp", "model")),
            P(("ens", "fsdp", "model")),
        ),
        out_specs=(P(("ens", "model"), None), P(("ens", "model"), None), P("ens")),
        check_vma=False,
    )
```
